512 devices in a mesh: seq: 64 (over z, x, y_hi), chan: 8 (over y_lo, core).
Axes of the slice: x: 4, y: 8 (y_hi: 2, y_lo: 4; y = y_hi * 4 + y_lo), z: 8, core: 2. Of those that a mesh axis runs over, the one named last changes fastest.
Arguments:
- values: bfloat16 [256, 32768], P('chan', 'seq'), may hold values from -6 to 6
- gate_one: bfloat16 [256, 32768], P('chan', 'seq'), may hold values from -6 to 6
- gate_two: bfloat16 [256, 32768], P('chan', 'seq'), may hold values from -6 to 6
- filter_one: float32 [256, 32768], P('chan', 'seq'), may hold values from -1 to 1
- filter_two: float32 [256, 32768], P('chan', 'seq'), may hold values from -1 to 1
- skip_one: float32 [256], P('chan'), may hold values from -1 to 1
- skip_two: float32 [256], P('chan'), may hold values from -1 to 1
- mix_weight: bfloat16 [256, 256], P(None, 'chan'), may hold values from -0.375 to 0.375
Outputs:
- mixed: bfloat16 [256, 32768], P('chan', 'seq')
The draws below stay inside these ranges and needn't reach their ends.
All inputs are finite; a program needn't handle non-finite values.
Results may differ from the reference program's by a relative error of at most 0.0051.
Values may be sent and summed in bfloat16 or wider, within the bound.
No kernel may reach another device: no remote copies, remote signals or barrier semaphores. Data moves between devices by JAX's collectives and lax.ppermute only.
A program may use at most 64 MiB of HBM per device.

```python
import math
import jax
import jax.numpy as jnp
from jax import lax

D = 256
SEQ_LEN = 32768


def filter_law(key):
    streams = jax.random.split(key, 6)
    sequence_locations = jnp.arange(SEQ_LEN, dtype=jnp.float32)[None, :]
    fast_share = 0.4
    chooser = jax.random.uniform(streams[0], (D, 1))
    quick = jnp.exp(jax.random.uniform(streams[1], (D, 1), minval=math.log(10.0), maxval=math.log(40.0)))
    gentle = jnp.exp(jax.random.uniform(streams[2], (D, 1), minval=math.log(1.0 * SEQ_LEN), maxval=math.log(8.0 * SEQ_LEN)))
    lengths_of = jnp.where(chooser < fast_share, quick, gentle)
    nominal_dimensions = -sequence_locations / lengths_of
    destination_places = jax.random.randint(streams[3], (D, 4), 0, SEQ_LEN)
    discarded_elements = jnp.log(jax.random.uniform(streams[4], (D, 4), minval=0.5, maxval=0.8))
    for contiguous_group_number in range(4):
        following_update = sequence_locations >= destination_places[:, contiguous_group_number:contiguous_group_number + 1].astype(jnp.float32)
        nominal_dimensions = nominal_dimensions + discarded_elements[:, contiguous_group_number:contiguous_group_number + 1] * following_update.astype(jnp.float32)
    envelope = jnp.exp(nominal_dimensions)
    rough = jax.random.normal(streams[5], (D, SEQ_LEN))
    reshaped_rows = rough * envelope
    return reshaped_rows / jnp.sqrt(jnp.sum(reshaped_rows * reshaped_rows, axis=1, keepdims=True))


def draw_filter_one(key, part):
    return filter_law(jax.random.fold_in(key, 11)).astype(jnp.float32)


def draw_filter_two(key, part):
    return filter_law(jax.random.fold_in(key, 23)).astype(jnp.float32)


def block_levels(key, shape, cuts, low, high):
    def one(dim, shards_of):
        draws = jax.random.uniform(jax.random.fold_in(jax.random.fold_in(key, 6), dim), (shards_of,), jnp.float32, low / len(cuts), high / len(cuts))
        return jnp.repeat(jnp.exp(draws), shape[dim] // shards_of).reshape((-1,) + (1,) * (len(shape) - dim - 1))

    loudness = one(*cuts[0])
    for cut in cuts[1:]:
        loudness = loudness * one(*cut)
    return loudness


def normal_values(stream_key, dims, scale, reach, cuts=(), kind=jnp.bfloat16):
    factor_of = block_levels(stream_key, dims, cuts, -0.22, 0.18) if cuts else 1.0
    values = jax.random.normal(stream_key, dims, jnp.float32) * scale * factor_of
    return jnp.minimum(jnp.maximum(values, -reach), reach).astype(kind)


def setup_inputs(seed: int = 0) -> dict:
    arg_keys = jax.random.split(jax.random.key(seed), 9)
    values = normal_values(arg_keys[0], (D, SEQ_LEN), 1.0, 6.0, ((0, 8), (1, 64)))
    gate_one = normal_values(arg_keys[1], (D, SEQ_LEN), 1.0, 6.0, ((0, 8), (1, 64)))
    gate_two = normal_values(arg_keys[2], (D, SEQ_LEN), 1.0, 6.0, ((0, 8), (1, 64)))
    filter_one = draw_filter_one(jax.random.fold_in(arg_keys[8], 71), 0)
    filter_two = draw_filter_two(jax.random.fold_in(arg_keys[8], 71), 0)
    skip_one = jnp.clip(jax.random.uniform(arg_keys[5], (D,), jnp.float32, -1.0, 1.0) * block_levels(arg_keys[5], (D,), ((0, 8),), -0.4, 0.0), -1.0, 1.0)
    skip_two = jnp.clip(jax.random.uniform(arg_keys[6], (D,), jnp.float32, -1.0, 1.0) * block_levels(arg_keys[6], (D,), ((0, 8),), -0.4, 0.0), -1.0, 1.0)
    mix_weight = normal_values(arg_keys[7], (D, D), D ** -0.5, 0.375, ((1, 8),))
    return dict(values=values, gate_one=gate_one, gate_two=gate_two, filter_one=filter_one, filter_two=filter_two, skip_one=skip_one, skip_two=skip_two, mix_weight=mix_weight)


def causal(signal, filter_taps):
    padded = 2 * signal.shape[-1]
    spectrum = jnp.fft.rfft(signal, n=padded) * jnp.fft.rfft(filter_taps, n=padded)
    return jnp.fft.irfft(spectrum, n=padded)[..., :signal.shape[-1]].astype(jnp.float32)


def channel_block(pieces):
    values, gate_one, gate_two, filter_one, filter_two, skip_one, skip_two = pieces
    values_wide = values.astype(jnp.float32)
    conv_one = causal(values_wide, filter_one)
    gated = gate_one.astype(jnp.float32) * (conv_one + skip_one[:, None] * values_wide)
    conv_two = causal(gated, filter_two)
    return (gate_two.astype(jnp.float32) * (conv_two + skip_two[:, None] * gated)).astype(jnp.bfloat16)


def reference(values, gate_one, gate_two, filter_one, filter_two, skip_one, skip_two, mix_weight):
    blocks_of = 8

    def by_block(source):
        return source.reshape((D // blocks_of, blocks_of) + source.shape[1:])

    stacked = tuple(by_block(source) for source in (values, gate_one, gate_two, filter_one, filter_two, skip_one, skip_two))
    mixed_in = lax.map(channel_block, stacked).reshape(D, SEQ_LEN)
    summed = jnp.dot(mix_weight.T, mixed_in, preferred_element_type=jnp.float32)
    return jax.nn.silu(summed).astype(jnp.bfloat16)
```

```python
import jax
import jax.numpy as jnp
from jax import lax
from jax.experimental import pallas as pl
from jax.experimental.pallas import tpu as pltpu
from jax.sharding import PartitionSpec as P

BLOCK = 128
SEQ_WAYS = 64
CHAN_WAYS = 8
OWN_CHANNELS = 32
OWN_BLOCKS = 4
ROWS = 18
BLOCKS = SEQ_WAYS * OWN_BLOCKS
HALF = BLOCKS // 2
SHIFTS = 16
GROUPS = BLOCKS // SHIFTS
F32 = jnp.float32
BF16 = jnp.bfloat16


def pack_kernel(values, gate_one, gate_two, filter_one, filter_two, send, wide):
    for half in range(2):
        base = half * OWN_CHANNELS * ROWS
        for kind, source in enumerate((values, filter_one, gate_one, filter_two)):
            for q in range(OWN_BLOCKS):
                piece = source[:, q * BLOCK : (q + 1) * BLOCK].astype(F32)
                wide[pl.ds(base + kind * OWN_BLOCKS + q, OWN_CHANNELS, stride=ROWS), :] = piece
        for u in range(2):
            q = 2 * u + half
            piece = gate_two[:, q * BLOCK : (q + 1) * BLOCK].astype(F32)
            wide[pl.ds(base + 4 * OWN_BLOCKS + u, OWN_CHANNELS, stride=ROWS), :] = piece
    send[...] = wide[...].astype(BF16)


def build_toeplitz(taps, table):
    lower = lax.broadcasted_iota(jnp.int32, (BLOCK, BLOCK), 1) >= lax.broadcasted_iota(
        jnp.int32, (BLOCK, BLOCK), 0
    )
    per_step = 8

    def step(i, before):
        start = pl.multiple_of(i * per_step, per_step)
        rows = taps[pl.ds(start, per_step), :]
        for j in range(per_step):
            spread = jnp.broadcast_to(rows[j : j + 1, :], (BLOCK, BLOCK))
            turned = pltpu.roll(spread, 0, 1, stride=1, stride_axis=0)
            at = pl.multiple_of((start + j) * BLOCK, BLOCK)
            table[pl.ds(at, BLOCK), :] = jnp.where(lower, turned, before).astype(BF16)
            before = turned
        return before

    lax.fori_loop(0, BLOCKS // per_step, step, jnp.zeros((BLOCK, BLOCK), F32))


def conv_kernel(
    skip_one, skip_two, recv, out, wide, x_pad, taps, gate, g_pad, g_turn, x_wide, table, g_wide, acc, out_wide
):
    place = lax.axis_index("seq")
    half = place // OWN_CHANNELS
    channel = place % OWN_CHANNELS
    first_skip = skip_one[channel]
    second_skip = skip_two[channel]
    pad = 32

    wide[...] = recv[...].astype(F32)
    x_pad[0:pad, :] = jnp.zeros((pad, BLOCK), F32)
    g_pad[0:pad, :] = jnp.zeros((pad, BLOCK), F32)
    for q in range(OWN_BLOCKS):
        def rows_of(kind):
            return wide[pl.ds(kind * OWN_BLOCKS + q, SEQ_WAYS, stride=ROWS), :]
        x_pad[pl.ds(pad + q, SEQ_WAYS, stride=OWN_BLOCKS), :] = rows_of(0)
        taps[pl.ds(q, SEQ_WAYS, stride=OWN_BLOCKS), :] = rows_of(1)
        gate[pl.ds(q, SEQ_WAYS, stride=OWN_BLOCKS), :] = rows_of(2)
        taps[pl.ds(BLOCKS + q, SEQ_WAYS, stride=OWN_BLOCKS), :] = rows_of(3)

    build_toeplitz(taps.at[0:BLOCKS], table)
    for b in range(SHIFTS):
        x_wide[:, b * BLOCK : (b + 1) * BLOCK] = x_pad[pad - b : pad - b + BLOCKS, :].astype(BF16)
    span = SHIFTS * BLOCK
    for a in range(GROUPS):
        top = SHIFTS * a
        part = jnp.dot(
            x_wide[0 : BLOCKS - top, :], table[a * span : (a + 1) * span, :], preferred_element_type=F32
        )
        if a == 0:
            acc[...] = part
        else:
            acc[top:BLOCKS, :] += part

    g_pad[pad : pad + BLOCKS, :] = gate[...] * (acc[...] + first_skip * x_pad[pad : pad + BLOCKS, :])
    is_odd = half == 1
    g_turn[1 : pad + BLOCKS, :] = jnp.where(
        is_odd, g_pad[1 : pad + BLOCKS, :], g_pad[0 : pad + BLOCKS - 1, :]
    )
    build_toeplitz(taps.at[BLOCKS : 2 * BLOCKS], table)
    for b in range(SHIFTS):
        for r in range(2):
            g_wide[:, (2 * b + r) * BLOCK : (2 * b + r + 1) * BLOCK] = g_turn[
                pl.ds(pad + 1 - r - 2 * b, HALF, stride=2), :
            ].astype(BF16)
    span = 2 * SHIFTS * BLOCK
    for a in range(HALF // SHIFTS):
        top = SHIFTS * a
        part = jnp.dot(
            g_wide[0 : HALF - top, :], table[a * span : (a + 1) * span, :], preferred_element_type=F32
        )
        if a == 0:
            acc[0:HALF, :] = part
        else:
            acc[top:HALF, :] += part
    for u in range(2):
        direct = g_turn[pl.ds(pad + 1 + 2 * u, SEQ_WAYS, stride=4), :]
        conv_two = acc[pl.ds(u, SEQ_WAYS, stride=2), :]
        second_gate = wide[pl.ds(4 * OWN_BLOCKS + u, SEQ_WAYS, stride=ROWS), :]
        mixed = second_gate * (conv_two + second_skip * direct)
        for c in range(CHAN_WAYS):
            out_wide[pl.ds(2 * c + u, SEQ_WAYS, stride=2 * CHAN_WAYS), :] = mixed
    out[...] = out_wide[...].astype(BF16)


def mix_kernel(weight, recv, out, weight_wide):
    for u in range(2):
        weight_wide[...] = jnp.zeros((4 * BLOCK, OWN_CHANNELS), F32)
        for c in range(CHAN_WAYS):
            weight_wide[pl.ds(2 * c + u, OWN_CHANNELS, stride=2 * CHAN_WAYS), :] = weight[
                c * OWN_CHANNELS : (c + 1) * OWN_CHANNELS, :
            ].astype(F32)
        picked = weight_wide[...].astype(BF16)
        for half in range(2):
            summed = lax.dot_general(
                picked,
                recv[half * 512 : (half + 1) * 512, :],
                (((0,), (0,)), ((), ())),
                preferred_element_type=F32,
            )
            q = 2 * u + half
            out[:, q * BLOCK : (q + 1) * BLOCK] = (summed / (1.0 + jnp.exp(-summed))).astype(BF16)


def per_device(values, gate_one, gate_two, filter_one, filter_two, skip_one, skip_two, mix_weight):
    whole = pl.BlockSpec(memory_space=pltpu.VMEM)
    scalars = pl.BlockSpec(memory_space=pltpu.SMEM)
    send = pl.pallas_call(
        pack_kernel,
        out_shape=jax.ShapeDtypeStruct((SEQ_WAYS * ROWS, BLOCK), BF16),
        in_specs=[whole] * 5,
        out_specs=whole,
        scratch_shapes=[pltpu.VMEM((SEQ_WAYS * ROWS, BLOCK), F32)],
        name="pack",
    )(values, gate_one, gate_two, filter_one, filter_two)
    recv = lax.all_to_all(
        send.reshape(SEQ_WAYS, ROWS // 2, 2, BLOCK), "seq", split_axis=0, concat_axis=0, tiled=True
    ).reshape(SEQ_WAYS * ROWS, BLOCK)
    spread = pl.pallas_call(
        conv_kernel,
        out_shape=jax.ShapeDtypeStruct((SEQ_WAYS * CHAN_WAYS * 2, BLOCK), BF16),
        in_specs=[scalars, scalars, whole],
        out_specs=whole,
        scratch_shapes=[
            pltpu.VMEM((SEQ_WAYS * ROWS, BLOCK), F32),
            pltpu.VMEM((32 + BLOCKS, BLOCK), F32),
            pltpu.VMEM((2 * BLOCKS, BLOCK), F32),
            pltpu.VMEM((BLOCKS, BLOCK), F32),
            pltpu.VMEM((32 + BLOCKS, BLOCK), F32),
            pltpu.VMEM((32 + BLOCKS, BLOCK), F32),
            pltpu.VMEM((BLOCKS, SHIFTS * BLOCK), BF16),
            pltpu.VMEM((BLOCKS * BLOCK, BLOCK), BF16),
            pltpu.VMEM((HALF, 2 * SHIFTS * BLOCK), BF16),
            pltpu.VMEM((BLOCKS, BLOCK), F32),
            pltpu.VMEM((SEQ_WAYS * CHAN_WAYS * 2, BLOCK), F32),
        ],
        name="convs",
    )(skip_one, skip_two, recv)
    gathered = lax.all_to_all(
        spread.reshape(SEQ_WAYS * CHAN_WAYS, 2, BLOCK),
        ("seq", "chan"),
        split_axis=0,
        concat_axis=0,
        tiled=True,
    ).reshape(SEQ_WAYS * CHAN_WAYS * 2, BLOCK)
    return pl.pallas_call(
        mix_kernel,
        out_shape=jax.ShapeDtypeStruct((OWN_CHANNELS, OWN_BLOCKS * BLOCK), BF16),
        in_specs=[whole, whole],
        out_specs=whole,
        scratch_shapes=[pltpu.VMEM((4 * BLOCK, OWN_CHANNELS), F32)],
        name="mix",
    )(mix_weight, gathered)


def solution(mesh):
    return jax.shard_map(
        per_device,
        mesh=mesh,
        in_specs=(
            P("chan", "seq"),
            P("chan", "seq"),
            P("chan", "seq"),
            P("chan", "seq"),
            P("chan", "seq"),
            P("chan"),
            P("chan"),
            P(None, "chan"),
        ),
        out_specs=P("chan", "seq"),
        check_vma=False,
    )
```

```python
import jax
import jax.numpy as jnp
from jax import lax
from jax.experimental import pallas as pl
from jax.experimental.pallas import tpu as pltpu
from jax.sharding import PartitionSpec as P

BLOCK = 128
PIECE = 64
SEQ_WAYS = 64
CHAN_WAYS = 8
OWN_CHANNELS = 32
OWN_BLOCKS = 4
ROWS = 20
BLOCKS = SEQ_WAYS * OWN_BLOCKS
LAGS = 128
SHIFTS = 8
PAD = 8
STEPS = 8
JOINED = 4
SPAN = SHIFTS * BLOCK
CHUNK = SPAN // PIECE
F32 = jnp.float32
BF16 = jnp.bfloat16


def swap(a):
    return pltpu.roll(a, PIECE, 1)


def join(low, high):
    return jnp.where(lax.broadcasted_iota(jnp.int32, low.shape, 1) < PIECE, low, high)


def pack_kernel(values, gate_one, gate_two, filter_one, filter_two, send, wide):
    for half in range(2):
        for kind, source in enumerate((values, filter_one, gate_one, filter_two, gate_two)):
            for q in range(OWN_BLOCKS):
                piece = source[:, q * BLOCK : (q + 1) * BLOCK].astype(F32)
                wide[pl.ds(half * ROWS + kind * OWN_BLOCKS + q, OWN_CHANNELS, stride=2 * ROWS), :] = piece
    send[...] = wide[...].astype(BF16)


def lay_taps(source, taps, turned, f):
    for c in range(2):
        top = PAD + 2 * c * LAGS // 2
        near = source[top : top + LAGS // 2, :]
        far = source[top + LAGS // 2 : top + LAGS, :]
        taps[2 * f + c, pl.ds(PAD, LAGS // 2, stride=2), :] = join(near, swap(far))
        taps[2 * f + c, pl.ds(PAD + 1, LAGS // 2, stride=2), :] = join(swap(near), far)
        last = source[top + LAGS // 2 - 1 : top + LAGS // 2, :]
        before = source[top - 1 : top, :]
        edge = join(swap(before), last)
        taps[2 * f + c, 0:PAD, :] = jnp.broadcast_to(edge, (PAD, BLOCK))
        turned[2 * f + c, 0 : PAD + LAGS, :] = swap(taps[2 * f + c, 0 : PAD + LAGS, :])
        for rows in (taps, turned):
            rows[2 * f + c, PAD + LAGS :, :] = jnp.zeros((CHUNK, BLOCK), F32)


def masks():
    lane = lax.broadcasted_iota(jnp.int32, (8, BLOCK), 1) % PIECE
    row = lax.broadcasted_iota(jnp.int32, (8, BLOCK), 0)
    return [lane < PIECE - 8 * m - row for m in range(PIECE // 8)]


def build_chunk(kept, taps, turned, f, lag, table, at, count=CHUNK):
    for k in range(count):
        for c in range(2):
            now = jnp.broadcast_to(taps[2 * f + c, pl.ds(lag + PAD + k, 1), :], (8, BLOCK))
            before = jnp.broadcast_to(turned[2 * f + c, pl.ds(lag + PAD + k - 1, 1), :], (8, BLOCK))
            tiles = [
                pltpu.roll(jnp.where(kept[m], now, before), 8 * m, 1, stride=1, stride_axis=0)
                for m in range(PIECE // 8)
            ]
            rows = pl.ds(at + k * PIECE, PIECE)
            table[rows, c * BLOCK : (c + 1) * BLOCK] = jnp.concatenate(tiles, axis=0).astype(BF16)


def side_by_side(pieces):
    return jnp.concatenate(pieces, axis=1)


def conv_kernel(
    skips, recv, out, wide, x_pad, h_one, h_two, gate, even, odd, taps, turned, x_wide, chunk_a, chunk_b, table_two, table_late,
    g_wide, acc, mixed, out_wide, spaced
):
    place = lax.axis_index("seq")
    half = place % 2
    tables_one = (chunk_a, chunk_b)
    channel = place // 2
    wide[...] = recv[...].astype(F32)
    for padded in (x_pad, h_one, h_two, even, odd):
        padded[0:PAD, :] = jnp.zeros((PAD, BLOCK), F32)
    x_wide[0 : 2 * PIECE, :] = jnp.zeros((2 * PIECE, SPAN), BF16)
    g_wide[:, 0:PIECE, :] = jnp.zeros((SHIFTS, PIECE, BLOCK), BF16)
    for q in range(OWN_BLOCKS):
        def rows_of(kind):
            return wide[pl.ds(kind * OWN_BLOCKS + q, SEQ_WAYS, stride=ROWS), :]
        x_pad[pl.ds(PAD + q, SEQ_WAYS, stride=OWN_BLOCKS), :] = rows_of(0)
        h_one[pl.ds(PAD + q, SEQ_WAYS, stride=OWN_BLOCKS), :] = rows_of(1)
        gate[pl.ds(q, SEQ_WAYS, stride=OWN_BLOCKS), :] = rows_of(2)
        h_two[pl.ds(PAD + q, SEQ_WAYS, stride=OWN_BLOCKS), :] = rows_of(3)

    lay_taps(h_one, taps, turned, 0)
    lay_taps(h_two, taps, turned, 1)
    kept = masks()
    build_chunk(kept, taps, turned, 0, 0, tables_one[0], 0)

    x_now = x_pad[PAD : PAD + BLOCKS, :]
    even[PAD : PAD + BLOCKS, :] = join(x_now, x_pad[PAD - 1 : PAD - 1 + BLOCKS, :])
    odd[PAD : PAD + BLOCKS, :] = swap(x_now)
    groups = BLOCKS // 8
    for b in range(SHIFTS):
        stacked = jnp.concatenate(
            [
                even[PAD - b : PAD - b + BLOCKS, :].reshape(groups, 8, BLOCK),
                odd[PAD - b : PAD - b + BLOCKS, :].reshape(groups, 8, BLOCK),
            ],
            axis=1,
        )
        x_wide[2 * PIECE : 2 * PIECE + 2 * BLOCKS, b * BLOCK : (b + 1) * BLOCK] = stacked.reshape(
            2 * BLOCKS, BLOCK
        ).astype(BF16)

    acc[...] = jnp.zeros((2 * BLOCKS, 2 * BLOCK), F32)

    def first_conv(i, carry):
        total = acc[...]
        for j in range(JOINED):
            a = i * JOINED + j
            total += jnp.dot(
                x_wide[pl.ds(pl.multiple_of(2 * PIECE - 16 * a, 16), 2 * BLOCKS), :],
                tables_one[j % 2][...],
                preferred_element_type=F32,
            )
            build_chunk(kept, taps, turned, 0, (a + 1) * CHUNK, tables_one[(j + 1) % 2], 0)
            at = pl.multiple_of(a * (SPAN // 2), SPAN // 2)
            build_chunk(kept, taps, turned, 1, a * (CHUNK // 2), table_two, at, CHUNK // 2)
        acc[...] = total
        return carry

    lax.fori_loop(0, STEPS // JOINED, first_conv, 0)

    def group(n, parity):
        at = 16 * n + 8 * parity
        total = acc[at : at + 8, 0:BLOCK]
        if n >= groups // 2:
            back = at - BLOCKS
            total = total + acc[back : back + 8, BLOCK : 2 * BLOCK]
        return total

    first_skip = skips[pl.ds(channel, 1), :]
    second_skip = skips[pl.ds(OWN_CHANNELS + channel, 1), :]
    is_odd = half == 1
    spaced[0 : 2 * PAD, :] = jnp.zeros((2 * PAD, BLOCK), F32)
    start = pl.multiple_of(2 * PAD - 8 * half, 8)
    for n in range(groups):
        here = [group(n, parity) for parity in range(2)]
        rows = slice(8 * n, 8 * n + 8)
        padded_rows = slice(PAD + 8 * n, PAD + 8 * n + 8)
        if n >= groups // 4:
            prior = [group(n - groups // 4, parity) for parity in range(2)]
        else:
            prior = [jnp.zeros((8, BLOCK), F32)] * 2
        conv_one = join(here[0], prior[1]) + swap(join(here[1], prior[0]))
        h_one[padded_rows, :] = gate[rows, :] * (conv_one + first_skip * x_pad[padded_rows, :])
    gated = h_one[PAD : PAD + BLOCKS, :]
    even[0:BLOCKS, :] = join(gated, h_one[PAD - 1 : PAD - 1 + BLOCKS, :])
    odd[0:BLOCKS, :] = swap(gated)
    for n in range(groups):
        spaced[pl.ds(start + 16 * n, 8, stride=2), :] = even[8 * n : 8 * n + 8, :]
        spaced[pl.ds(start + 16 * n + 1, 8, stride=2), :] = odd[8 * n : 8 * n + 8, :]
    for b in range(SHIFTS):
        picked = [spaced[2 * PAD + 16 * n - 2 * b : 2 * PAD + 16 * n - 2 * b + 8, :] for n in range(groups)]
        if b == 0:
            even[0:BLOCKS, :] = jnp.concatenate(picked, axis=0)
        g_wide[b, PIECE : PIECE + BLOCKS, :] = jnp.concatenate(picked, axis=0).astype(BF16)
    total = None
    for a in range(STEPS):
        early = a < STEPS // 2
        at = (a % (STEPS // 2)) * SPAN
        part = jnp.dot(
            side_by_side([g_wide[b, PIECE - 8 * a : PIECE - 8 * a + BLOCKS, :] for b in range(SHIFTS)]),
            (table_two if early else table_late)[at : at + SPAN, :],
            preferred_element_type=F32,
        )
        if early:
            build_chunk(kept, taps, turned, 1, LAGS // 2 + a * CHUNK, table_late, at)
        total = part if a == 0 else total + part
        if a == STEPS // 2 - 1 or a == STEPS - 1:
            acc[0:BLOCKS, :] = total
            total = acc[0:BLOCKS, :]

    mixed[0:LAGS, :] = acc[0:LAGS, 0:BLOCK]
    mixed[LAGS:BLOCKS, :] = acc[LAGS:BLOCKS, 0:BLOCK] + acc[0:LAGS, BLOCK : 2 * BLOCK]
    gate[0:PIECE, :] = mixed[0:PIECE, :] + second_skip * even[0:PIECE, :]
    gate[PIECE:BLOCKS, :] = (
        mixed[PIECE:BLOCKS, :] + swap(mixed[0 : BLOCKS - PIECE, :]) + second_skip * even[PIECE:BLOCKS, :]
    )
    for u in range(OWN_BLOCKS):
        low = gate[pl.ds(2 * u, OWN_CHANNELS, stride=8), :]
        high = gate[pl.ds(2 * u + 1, OWN_CHANNELS, stride=8), :]
        gates = [wide[pl.ds(p * ROWS + 4 * OWN_BLOCKS + u, OWN_CHANNELS, stride=2 * ROWS), :] for p in range(2)]
        result = jnp.where(is_odd, gates[1], gates[0]) * join(low, swap(high))
        for copy in range(2):
            out_wide[pl.ds(OWN_BLOCKS * copy + u, OWN_CHANNELS, stride=2 * OWN_BLOCKS), :] = result
    for n in range(OWN_CHANNELS):
        once = out_wide[8 * n : 8 * n + 8, :]
        twice = jnp.concatenate([once, once], axis=0).astype(BF16)
        for copy in range(2):
            out[32 * n + 16 * copy : 32 * n + 16 * copy + 16, :] = twice


def side_kernel(weight, skip_one, skip_two, out, skips, spread):
    square = (OWN_CHANNELS, OWN_CHANNELS)
    same = lax.broadcasted_iota(jnp.int32, square, 0) == lax.broadcasted_iota(jnp.int32, square, 1)
    for i, skip in enumerate((skip_one, skip_two)):
        column = jnp.sum(jnp.where(same, jnp.broadcast_to(skip[...], square), 0.0), axis=1, keepdims=True)
        skips[i * OWN_CHANNELS : (i + 1) * OWN_CHANNELS, :] = jnp.broadcast_to(column, (OWN_CHANNELS, BLOCK))
    quarter = lax.broadcasted_iota(jnp.int32, (OWN_CHANNELS, BLOCK), 1) // OWN_CHANNELS
    for c in range(CHAN_WAYS):
        own = weight[c * OWN_CHANNELS : (c + 1) * OWN_CHANNELS, :].astype(F32)
        repeated = jnp.concatenate([own] * OWN_BLOCKS, axis=1)
        for u in range(OWN_BLOCKS):
            spread[pl.ds(OWN_BLOCKS * c + u, OWN_CHANNELS, stride=OWN_BLOCKS * CHAN_WAYS), :] = jnp.where(
                quarter == u, repeated, 0.0
            )
    out[...] = spread[...].astype(BF16)


def mix_kernel(weight, recv, out):
    summed = lax.dot_general(weight[...], recv[...], (((0,), (0,)), ((), ())), preferred_element_type=F32)
    active = (summed / (1.0 + jnp.exp(-summed))).astype(BF16)
    for u in range(OWN_BLOCKS):
        out[:, u * BLOCK : (u + 1) * BLOCK] = active[u * OWN_CHANNELS : (u + 1) * OWN_CHANNELS, :]


def per_device(values, gate_one, gate_two, filter_one, filter_two, skip_one, skip_two, mix_weight):
    whole = pl.BlockSpec(memory_space=pltpu.VMEM)
    send = pl.pallas_call(
        pack_kernel,
        out_shape=jax.ShapeDtypeStruct((SEQ_WAYS * ROWS, BLOCK), BF16),
        in_specs=[whole] * 5,
        out_specs=whole,
        scratch_shapes=[pltpu.VMEM((SEQ_WAYS * ROWS, BLOCK), F32)],
        name="pack",
    )(values, gate_one, gate_two, filter_one, filter_two)
    recv = lax.all_to_all(
        send.reshape(SEQ_WAYS, ROWS // 2, 2, BLOCK), "seq", split_axis=0, concat_axis=0, tiled=True
    ).reshape(SEQ_WAYS * ROWS, BLOCK)
    laid_weight, skips = pl.pallas_call(
        side_kernel,
        out_shape=(
            jax.ShapeDtypeStruct((OWN_CHANNELS * CHAN_WAYS * OWN_BLOCKS, BLOCK), BF16),
            jax.ShapeDtypeStruct((2 * OWN_CHANNELS, BLOCK), F32),
        ),
        in_specs=[whole] * 3,
        out_specs=(whole, whole),
        scratch_shapes=[pltpu.VMEM((OWN_CHANNELS * CHAN_WAYS * OWN_BLOCKS, BLOCK), F32)],
        compiler_params=pltpu.CompilerParams(vmem_limit_bytes=8 << 20),
        name="side",
    )(mix_weight, skip_one.reshape(1, OWN_CHANNELS), skip_two.reshape(1, OWN_CHANNELS))
    spread = pl.pallas_call(
        conv_kernel,
        out_shape=jax.ShapeDtypeStruct((SEQ_WAYS * CHAN_WAYS * 2, BLOCK), BF16),
        in_specs=[whole, whole],
        out_specs=whole,
        scratch_shapes=[
            pltpu.VMEM((SEQ_WAYS * ROWS, BLOCK), F32),
            pltpu.VMEM((PAD + BLOCKS, BLOCK), F32),
            pltpu.VMEM((PAD + BLOCKS, BLOCK), F32),
            pltpu.VMEM((PAD + BLOCKS, BLOCK), F32),
            pltpu.VMEM((BLOCKS, BLOCK), F32),
            pltpu.VMEM((PAD + BLOCKS, BLOCK), F32),
            pltpu.VMEM((PAD + BLOCKS, BLOCK), F32),
            pltpu.VMEM((4, PAD + LAGS + CHUNK, BLOCK), F32),
            pltpu.VMEM((4, PAD + LAGS + CHUNK, BLOCK), F32),
            pltpu.VMEM((2 * PIECE + 2 * BLOCKS, SPAN), BF16),
            pltpu.VMEM((SPAN, 2 * BLOCK), BF16),
            pltpu.VMEM((SPAN, 2 * BLOCK), BF16),
            pltpu.VMEM((LAGS // 2 * PIECE, 2 * BLOCK), BF16),
            pltpu.VMEM((LAGS // 2 * PIECE, 2 * BLOCK), BF16),
            pltpu.VMEM((SHIFTS, PIECE + BLOCKS, BLOCK), BF16),
            pltpu.VMEM((2 * BLOCKS, 2 * BLOCK), F32),
            pltpu.VMEM((BLOCKS, BLOCK), F32),
            pltpu.VMEM((BLOCKS, BLOCK), F32),
            pltpu.VMEM((2 * PAD + 2 * BLOCKS, BLOCK), F32),
        ],
        compiler_params=pltpu.CompilerParams(vmem_limit_bytes=32 << 20),
        name="convs",
    )(skips, recv)
    gathered = lax.all_to_all(
        spread.reshape(OWN_CHANNELS * CHAN_WAYS, OWN_BLOCKS // 2, 2, BLOCK),
        ("seq", "chan"),
        split_axis=0,
        concat_axis=0,
        tiled=True,
        axis_index_groups=[
            [(2 * k + half) * CHAN_WAYS + c for k in range(OWN_CHANNELS) for c in range(CHAN_WAYS)] for half in range(2)
        ],
    ).reshape(SEQ_WAYS * CHAN_WAYS * 2, BLOCK)
    return pl.pallas_call(
        mix_kernel,
        out_shape=jax.ShapeDtypeStruct((OWN_CHANNELS, OWN_BLOCKS * BLOCK), BF16),
        in_specs=[whole, whole],
        out_specs=whole,
        compiler_params=pltpu.CompilerParams(vmem_limit_bytes=8 << 20),
        name="mix",
    )(laid_weight, gathered)


def solution(mesh):
    return jax.shard_map(
        per_device,
        mesh=mesh,
        in_specs=(
            P("chan", "seq"),
            P("chan", "seq"),
            P("chan", "seq"),
            P("chan", "seq"),
            P("chan", "seq"),
            P("chan"),
            P("chan"),
            P(None, "chan"),
        ),
        out_specs=P("chan", "seq"),
        check_vma=False,
    )
```

```python
import jax
import jax.numpy as jnp
from jax import lax
from jax.experimental import pallas as pl
from jax.experimental.pallas import tpu as pltpu
from jax.sharding import PartitionSpec as P

BLOCK = 128
PIECE = 64
SEQ_WAYS = 64
CHAN_WAYS = 8
OWN_CHANNELS = 32
OWN_BLOCKS = 4
ROWS = 20
BLOCKS = SEQ_WAYS * OWN_BLOCKS
LAGS = 128
SHIFTS = 8
PAD = 8
STEPS = 8
JOINED = 4
SPAN = SHIFTS * BLOCK
CHUNK = SPAN // PIECE
F32 = jnp.float32
BF16 = jnp.bfloat16


def swap(a):
    return pltpu.roll(a, PIECE, 1)


def join(low, high):
    return jnp.where(lax.broadcasted_iota(jnp.int32, low.shape, 1) < PIECE, low, high)


def pack_kernel(values, gate_one, gate_two, filter_one, filter_two, send, wide, narrow, broad, ready, arrived, left):
    places = (
        (filter_one, broad.at[0], 1),
        (filter_two, broad.at[1], 3),
        (values, narrow.at[0], 0),
        (gate_one, narrow.at[1], 2),
        (gate_two, narrow.at[2], 4),
    )
    fetches = [pltpu.make_async_copy(source, local, arrived.at[i]) for i, (source, local, _) in enumerate(places)]
    for fetch in fetches:
        fetch.start()
    for fetch, (_, local, kind) in zip(fetches, places):
        fetch.wait()
        for q in range(OWN_BLOCKS):
            piece = local[:, q * BLOCK : (q + 1) * BLOCK].astype(F32)
            for half in range(2):
                wide[pl.ds(half * ROWS + kind * OWN_BLOCKS + q, OWN_CHANNELS, stride=2 * ROWS), :] = piece
    part = SEQ_WAYS * ROWS // 2
    sends = []
    for i in range(2):
        rows = pl.ds(i * part, part)
        ready[rows, :] = wide[rows, :].astype(BF16)
        sends.append(pltpu.make_async_copy(ready.at[rows], send.at[rows], left.at[i]))
        sends[i].start()
    for one in sends:
        one.wait()


def lay_taps(source, taps, turned, f):
    for c in range(2):
        top = PAD + 2 * c * LAGS // 2
        near = source[top : top + LAGS // 2, :]
        far = source[top + LAGS // 2 : top + LAGS, :]
        taps[2 * f + c, pl.ds(PAD, LAGS // 2, stride=2), :] = join(near, swap(far))
        taps[2 * f + c, pl.ds(PAD + 1, LAGS // 2, stride=2), :] = join(swap(near), far)
        last = source[top + LAGS // 2 - 1 : top + LAGS // 2, :]
        before = source[top - 1 : top, :]
        edge = join(swap(before), last)
        taps[2 * f + c, 0:PAD, :] = jnp.broadcast_to(edge, (PAD, BLOCK))
        turned[2 * f + c, 0 : PAD + LAGS, :] = swap(taps[2 * f + c, 0 : PAD + LAGS, :])
        for rows in (taps, turned):
            rows[2 * f + c, PAD + LAGS :, :] = jnp.zeros((CHUNK, BLOCK), F32)


def masks():
    lane = lax.broadcasted_iota(jnp.int32, (8, BLOCK), 1) % PIECE
    row = lax.broadcasted_iota(jnp.int32, (8, BLOCK), 0)
    return [lane < PIECE - 8 * m - row for m in range(PIECE // 8)]


def build_chunk(kept, taps, turned, f, lag, table, at, count=CHUNK):
    for k in range(count):
        for c in range(2):
            now = jnp.broadcast_to(taps[2 * f + c, pl.ds(lag + PAD + k, 1), :], (8, BLOCK))
            before = jnp.broadcast_to(turned[2 * f + c, pl.ds(lag + PAD + k - 1, 1), :], (8, BLOCK))
            tiles = [
                pltpu.roll(jnp.where(kept[m], now, before), 8 * m, 1, stride=1, stride_axis=0)
                for m in range(PIECE // 8)
            ]
            rows = pl.ds(at + k * PIECE, PIECE)
            table[rows, c * BLOCK : (c + 1) * BLOCK] = jnp.concatenate(tiles, axis=0).astype(BF16)


def side_by_side(pieces):
    return jnp.concatenate(pieces, axis=1)


def conv_kernel(
    skips, recv, out, wide, x_pad, h_one, h_two, gate, even, odd, taps, turned, x_wide, chunk_a, chunk_b, table_two, table_late,
    g_wide, acc, mixed, out_wide, spaced
):
    place = lax.axis_index("seq")
    half = place % 2
    tables_one = (chunk_a, chunk_b)
    channel = place // 2
    wide[...] = recv[...].astype(F32)
    for padded in (x_pad, h_one, h_two, even, odd):
        padded[0:PAD, :] = jnp.zeros((PAD, BLOCK), F32)
    x_wide[0 : 2 * PIECE, :] = jnp.zeros((2 * PIECE, SPAN), BF16)
    g_wide[:, 0:PIECE, :] = jnp.zeros((SHIFTS, PIECE, BLOCK), BF16)
    for q in range(OWN_BLOCKS):
        def rows_of(kind):
            return wide[pl.ds(kind * OWN_BLOCKS + q, SEQ_WAYS, stride=ROWS), :]
        x_pad[pl.ds(PAD + q, SEQ_WAYS, stride=OWN_BLOCKS), :] = rows_of(0)
        h_one[pl.ds(PAD + q, SEQ_WAYS, stride=OWN_BLOCKS), :] = rows_of(1)
        gate[pl.ds(q, SEQ_WAYS, stride=OWN_BLOCKS), :] = rows_of(2)
        h_two[pl.ds(PAD + q, SEQ_WAYS, stride=OWN_BLOCKS), :] = rows_of(3)

    lay_taps(h_one, taps, turned, 0)
    lay_taps(h_two, taps, turned, 1)
    kept = masks()
    build_chunk(kept, taps, turned, 0, 0, tables_one[0], 0)

    x_now = x_pad[PAD : PAD + BLOCKS, :]
    even[PAD : PAD + BLOCKS, :] = join(x_now, x_pad[PAD - 1 : PAD - 1 + BLOCKS, :])
    odd[PAD : PAD + BLOCKS, :] = swap(x_now)
    groups = BLOCKS // 8
    for b in range(SHIFTS):
        stacked = jnp.concatenate(
            [
                even[PAD - b : PAD - b + BLOCKS, :].reshape(groups, 8, BLOCK),
                odd[PAD - b : PAD - b + BLOCKS, :].reshape(groups, 8, BLOCK),
            ],
            axis=1,
        )
        x_wide[2 * PIECE : 2 * PIECE + 2 * BLOCKS, b * BLOCK : (b + 1) * BLOCK] = stacked.reshape(
            2 * BLOCKS, BLOCK
        ).astype(BF16)

    acc[...] = jnp.zeros((2 * BLOCKS, 2 * BLOCK), F32)

    def first_conv(i, carry):
        total = acc[...]
        for j in range(JOINED):
            a = i * JOINED + j
            total += jnp.dot(
                x_wide[pl.ds(pl.multiple_of(2 * PIECE - 16 * a, 16), 2 * BLOCKS), :],
                tables_one[j % 2][...],
                preferred_element_type=F32,
            )
            build_chunk(kept, taps, turned, 0, (a + 1) * CHUNK, tables_one[(j + 1) % 2], 0)
            at = pl.multiple_of(a * (SPAN // 2), SPAN // 2)
            build_chunk(kept, taps, turned, 1, a * (CHUNK // 2), table_two, at, CHUNK // 2)
        acc[...] = total
        return carry

    lax.fori_loop(0, STEPS // JOINED, first_conv, 0)

    def group(n, parity):
        at = 16 * n + 8 * parity
        total = acc[at : at + 8, 0:BLOCK]
        if n >= groups // 2:
            back = at - BLOCKS
            total = total + acc[back : back + 8, BLOCK : 2 * BLOCK]
        return total

    first_skip = skips[pl.ds(channel, 1), :]
    second_skip = skips[pl.ds(OWN_CHANNELS + channel, 1), :]
    is_odd = half == 1
    spaced[0 : 2 * PAD, :] = jnp.zeros((2 * PAD, BLOCK), F32)
    start = pl.multiple_of(2 * PAD - 8 * half, 8)
    for n in range(groups):
        here = [group(n, parity) for parity in range(2)]
        rows = slice(8 * n, 8 * n + 8)
        padded_rows = slice(PAD + 8 * n, PAD + 8 * n + 8)
        if n >= groups // 4:
            prior = [group(n - groups // 4, parity) for parity in range(2)]
        else:
            prior = [jnp.zeros((8, BLOCK), F32)] * 2
        conv_one = join(here[0], prior[1]) + swap(join(here[1], prior[0]))
        h_one[padded_rows, :] = gate[rows, :] * (conv_one + first_skip * x_pad[padded_rows, :])
    gated = h_one[PAD : PAD + BLOCKS, :]
    even[0:BLOCKS, :] = join(gated, h_one[PAD - 1 : PAD - 1 + BLOCKS, :])
    odd[0:BLOCKS, :] = swap(gated)
    for n in range(groups):
        spaced[pl.ds(start + 16 * n, 8, stride=2), :] = even[8 * n : 8 * n + 8, :]
        spaced[pl.ds(start + 16 * n + 1, 8, stride=2), :] = odd[8 * n : 8 * n + 8, :]
    for b in range(SHIFTS):
        picked = [spaced[2 * PAD + 16 * n - 2 * b : 2 * PAD + 16 * n - 2 * b + 8, :] for n in range(groups)]
        if b == 0:
            even[0:BLOCKS, :] = jnp.concatenate(picked, axis=0)
        g_wide[b, PIECE : PIECE + BLOCKS, :] = jnp.concatenate(picked, axis=0).astype(BF16)
    total = None
    for a in range(STEPS):
        early = a < STEPS // 2
        at = (a % (STEPS // 2)) * SPAN
        part = jnp.dot(
            side_by_side([g_wide[b, PIECE - 8 * a : PIECE - 8 * a + BLOCKS, :] for b in range(SHIFTS)]),
            (table_two if early else table_late)[at : at + SPAN, :],
            preferred_element_type=F32,
        )
        if early:
            build_chunk(kept, taps, turned, 1, LAGS // 2 + a * CHUNK, table_late, at)
        total = part if a == 0 else total + part
        if a == STEPS // 2 - 1 or a == STEPS - 1:
            acc[0:BLOCKS, :] = total
            total = acc[0:BLOCKS, :]

    mixed[0:LAGS, :] = acc[0:LAGS, 0:BLOCK]
    mixed[LAGS:BLOCKS, :] = acc[LAGS:BLOCKS, 0:BLOCK] + acc[0:LAGS, BLOCK : 2 * BLOCK]
    gate[0:PIECE, :] = mixed[0:PIECE, :] + second_skip * even[0:PIECE, :]
    gate[PIECE:BLOCKS, :] = (
        mixed[PIECE:BLOCKS, :] + swap(mixed[0 : BLOCKS - PIECE, :]) + second_skip * even[PIECE:BLOCKS, :]
    )
    for u in range(OWN_BLOCKS):
        low = gate[pl.ds(2 * u, OWN_CHANNELS, stride=8), :]
        high = gate[pl.ds(2 * u + 1, OWN_CHANNELS, stride=8), :]
        gates = [wide[pl.ds(p * ROWS + 4 * OWN_BLOCKS + u, OWN_CHANNELS, stride=2 * ROWS), :] for p in range(2)]
        result = jnp.where(is_odd, gates[1], gates[0]) * join(low, swap(high))
        for copy in range(2):
            out_wide[pl.ds(OWN_BLOCKS * copy + u, OWN_CHANNELS, stride=2 * OWN_BLOCKS), :] = result
    for n in range(OWN_CHANNELS):
        once = out_wide[8 * n : 8 * n + 8, :]
        twice = jnp.concatenate([once, once], axis=0).astype(BF16)
        for copy in range(2):
            out[32 * n + 16 * copy : 32 * n + 16 * copy + 16, :] = twice


def side_kernel(weight, skip_one, skip_two, out, skips, spread):
    square = (OWN_CHANNELS, OWN_CHANNELS)
    same = lax.broadcasted_iota(jnp.int32, square, 0) == lax.broadcasted_iota(jnp.int32, square, 1)
    for i, skip in enumerate((skip_one, skip_two)):
        column = jnp.sum(jnp.where(same, jnp.broadcast_to(skip[...], square), 0.0), axis=1, keepdims=True)
        skips[i * OWN_CHANNELS : (i + 1) * OWN_CHANNELS, :] = jnp.broadcast_to(column, (OWN_CHANNELS, BLOCK))
    quarter = lax.broadcasted_iota(jnp.int32, (OWN_CHANNELS, BLOCK), 1) // OWN_CHANNELS
    for c in range(CHAN_WAYS):
        own = weight[c * OWN_CHANNELS : (c + 1) * OWN_CHANNELS, :].astype(F32)
        repeated = jnp.concatenate([own] * OWN_BLOCKS, axis=1)
        for u in range(OWN_BLOCKS):
            spread[pl.ds(OWN_BLOCKS * c + u, OWN_CHANNELS, stride=OWN_BLOCKS * CHAN_WAYS), :] = jnp.where(
                quarter == u, repeated, 0.0
            )
    out[...] = spread[...].astype(BF16)


def mix_kernel(weight, recv, out):
    summed = lax.dot_general(weight[...], recv[...], (((0,), (0,)), ((), ())), preferred_element_type=F32)
    active = (summed / (1.0 + jnp.exp(-summed))).astype(BF16)
    for u in range(OWN_BLOCKS):
        out[:, u * BLOCK : (u + 1) * BLOCK] = active[u * OWN_CHANNELS : (u + 1) * OWN_CHANNELS, :]


def per_device(values, gate_one, gate_two, filter_one, filter_two, skip_one, skip_two, mix_weight):
    whole = pl.BlockSpec(memory_space=pltpu.VMEM)
    outside = pl.BlockSpec(memory_space=pl.ANY)
    send = pl.pallas_call(
        pack_kernel,
        out_shape=jax.ShapeDtypeStruct((SEQ_WAYS * ROWS, BLOCK), BF16),
        in_specs=[outside] * 5,
        out_specs=outside,
        scratch_shapes=[
            pltpu.VMEM((SEQ_WAYS * ROWS, BLOCK), F32),
            pltpu.VMEM((3, OWN_CHANNELS, OWN_BLOCKS * BLOCK), BF16),
            pltpu.VMEM((2, OWN_CHANNELS, OWN_BLOCKS * BLOCK), F32),
            pltpu.VMEM((SEQ_WAYS * ROWS, BLOCK), BF16),
            pltpu.SemaphoreType.DMA((5,)),
            pltpu.SemaphoreType.DMA((2,)),
        ],
        name="pack",
    )(values, gate_one, gate_two, filter_one, filter_two)
    recv = lax.all_to_all(
        send.reshape(SEQ_WAYS, ROWS // 2, 2, BLOCK), "seq", split_axis=0, concat_axis=0, tiled=True
    ).reshape(SEQ_WAYS * ROWS, BLOCK)
    laid_weight, skips = pl.pallas_call(
        side_kernel,
        out_shape=(
            jax.ShapeDtypeStruct((OWN_CHANNELS * CHAN_WAYS * OWN_BLOCKS, BLOCK), BF16),
            jax.ShapeDtypeStruct((2 * OWN_CHANNELS, BLOCK), F32),
        ),
        in_specs=[whole] * 3,
        out_specs=(whole, whole),
        scratch_shapes=[pltpu.VMEM((OWN_CHANNELS * CHAN_WAYS * OWN_BLOCKS, BLOCK), F32)],
        compiler_params=pltpu.CompilerParams(vmem_limit_bytes=8 << 20),
        name="side",
    )(mix_weight, skip_one.reshape(1, OWN_CHANNELS), skip_two.reshape(1, OWN_CHANNELS))
    spread = pl.pallas_call(
        conv_kernel,
        out_shape=jax.ShapeDtypeStruct((SEQ_WAYS * CHAN_WAYS * 2, BLOCK), BF16),
        in_specs=[whole, whole],
        out_specs=whole,
        scratch_shapes=[
            pltpu.VMEM((SEQ_WAYS * ROWS, BLOCK), F32),
            pltpu.VMEM((PAD + BLOCKS, BLOCK), F32),
            pltpu.VMEM((PAD + BLOCKS, BLOCK), F32),
            pltpu.VMEM((PAD + BLOCKS, BLOCK), F32),
            pltpu.VMEM((BLOCKS, BLOCK), F32),
            pltpu.VMEM((PAD + BLOCKS, BLOCK), F32),
            pltpu.VMEM((PAD + BLOCKS, BLOCK), F32),
            pltpu.VMEM((4, PAD + LAGS + CHUNK, BLOCK), F32),
            pltpu.VMEM((4, PAD + LAGS + CHUNK, BLOCK), F32),
            pltpu.VMEM((2 * PIECE + 2 * BLOCKS, SPAN), BF16),
            pltpu.VMEM((SPAN, 2 * BLOCK), BF16),
            pltpu.VMEM((SPAN, 2 * BLOCK), BF16),
            pltpu.VMEM((LAGS // 2 * PIECE, 2 * BLOCK), BF16),
            pltpu.VMEM((LAGS // 2 * PIECE, 2 * BLOCK), BF16),
            pltpu.VMEM((SHIFTS, PIECE + BLOCKS, BLOCK), BF16),
            pltpu.VMEM((2 * BLOCKS, 2 * BLOCK), F32),
            pltpu.VMEM((BLOCKS, BLOCK), F32),
            pltpu.VMEM((BLOCKS, BLOCK), F32),
            pltpu.VMEM((2 * PAD + 2 * BLOCKS, BLOCK), F32),
        ],
        compiler_params=pltpu.CompilerParams(vmem_limit_bytes=32 << 20),
        name="convs",
    )(skips, recv)
    gathered = lax.all_to_all(
        spread.reshape(OWN_CHANNELS * CHAN_WAYS, OWN_BLOCKS // 2, 2, BLOCK),
        ("seq", "chan"),
        split_axis=0,
        concat_axis=0,
        tiled=True,
        axis_index_groups=[
            [(2 * k + half) * CHAN_WAYS + c for k in range(OWN_CHANNELS) for c in range(CHAN_WAYS)] for half in range(2)
        ],
    ).reshape(SEQ_WAYS * CHAN_WAYS * 2, BLOCK)
    return pl.pallas_call(
        mix_kernel,
        out_shape=jax.ShapeDtypeStruct((OWN_CHANNELS, OWN_BLOCKS * BLOCK), BF16),
        in_specs=[whole, whole],
        out_specs=whole,
        compiler_params=pltpu.CompilerParams(vmem_limit_bytes=8 << 20),
        name="mix",
    )(laid_weight, gathered)


def solution(mesh):
    return jax.shard_map(
        per_device,
        mesh=mesh,
        in_specs=(
            P("chan", "seq"),
            P("chan", "seq"),
            P("chan", "seq"),
            P("chan", "seq"),
            P("chan", "seq"),
            P("chan"),
            P("chan"),
            P(None, "chan"),
        ),
        out_specs=P("chan", "seq"),
        check_vma=False,
    )
```
